32 devices in a mesh: leaf: 32 (over z, y, x, core).
Axes of the slice: x: 2, y: 2, z: 4, core: 2. Of those that a mesh axis runs over, the one named last changes fastest.
Arguments:
- leaf_inverses: float32 [32768, 1024], P('leaf'), may hold values from -1 to 1, as said below
- u_bases: float32 [32768, 320], P('leaf'), may hold values from -6 to 6
- v_bases: float32 [32768, 320], P('leaf'), may hold values from -6 to 6
- right_side: float32 [32768, 128], P('leaf'), may hold values from -6 to 6
Outputs:
- solution: float32 [32768, 128], P('leaf')
The draws below stay inside these ranges and needn't reach their ends.
Inputs may be any that keep to these rules, and one draw needn't show every extreme that they name: `leaf_inverses`: every run of 1024 rows starting at a multiple of 1024 is the inverse of a symmetric positive definite 1024 x 1024 matrix.
All inputs are finite; a program needn't handle non-finite values.
Results may differ from the reference program's by a relative error of at most 0.00014.
Values sent between devices are 32-bit elements; how exact they have to be, the bound alone decides.
A program may use at most 64 MiB of HBM per device.

```python
import jax
import jax.numpy as jnp
import numpy as np
from jax import lax

LEAF = 1024
RANK = 64
RHS = 128
LEVELS = 5
ROWS = 32768
N_LEAF = 32


def draw_leaf_inverses(key, part):
    noise_key, diag_key = jax.random.split(jax.random.fold_in(key, 11))
    noise = jnp.clip(jax.random.normal(noise_key, (N_LEAF, LEAF, LEAF), jnp.float32), -6.0, 6.0)
    symmetric = (noise + jnp.swapaxes(noise, 1, 2)) * (0.5 / jnp.sqrt(2.0 * LEAF))
    diagonal = jnp.exp(jax.random.uniform(diag_key, (N_LEAF, LEAF), jnp.float32, jnp.log(3.0), jnp.log(5.5)))
    blocks = symmetric + diagonal[:, :, None] * jnp.eye(LEAF, dtype=jnp.float32)[None]
    inverses = jnp.linalg.inv(blocks)
    inverses = 0.5 * (inverses + jnp.swapaxes(inverses, 1, 2))
    return inverses.reshape(N_LEAF * LEAF, LEAF).astype(jnp.float32)


def draw_bases(key):
    left_key, extra_key, weight_key = jax.random.split(jax.random.fold_in(key, 23), 3)
    columns = LEVELS * RANK
    left_rows = jnp.clip(jax.random.normal(left_key, (ROWS, columns), jnp.float32), -6.0, 6.0)
    extra_rows = jnp.clip(jax.random.normal(extra_key, (ROWS, columns), jnp.float32), -6.0, 6.0)
    coupling = jax.random.uniform(weight_key, (columns,), jnp.float32, 0.8, 1.3)
    right_rows = jnp.clip(coupling[None, :] * left_rows + 0.5 * extra_rows, -6.0, 6.0)
    return (left_rows, right_rows)


def draw_u_bases(key, part):
    return draw_bases(key)[0].astype(jnp.float32)


def draw_v_bases(key, part):
    return draw_bases(key)[1].astype(jnp.float32)


def shard_levels(key, extent, cuts, smallest, high):
    loudness = 1.0
    for position, parts in cuts:
        heights = jax.random.uniform(jax.random.fold_in(jax.random.fold_in(key, 6), position), (parts,), jnp.float32, smallest / len(cuts), high / len(cuts))
        loudness = loudness * jnp.repeat(jnp.exp(heights), extent[position] // parts).reshape((-1,) + (1,) * (len(extent) - 1 - position))
    return loudness


def bell_draw(rng, shape, width, limit, shards=(), held_as=jnp.bfloat16):
    result = jax.random.normal(rng, shape, jnp.float32) * width
    if len(shards) > 0:
        result = shard_levels(rng, shape, shards, -0.22, 0.18) * result
    return jnp.clip(result, min=-limit, max=limit).astype(held_as)


def setup_inputs(seed: int = 0) -> dict:
    keys = jax.random.split(jax.random.key(seed), 5)
    return {
        "leaf_inverses": draw_leaf_inverses(jax.random.fold_in(keys[4], 71), 0),
        "u_bases": draw_u_bases(jax.random.fold_in(keys[4], 71), 0),
        "v_bases": draw_v_bases(jax.random.fold_in(keys[4], 71), 0),
        "right_side": bell_draw(keys[3], (ROWS, RHS), 1.0, 6.0, ((0, 32),), jnp.float32),
    }


PRECISE = lax.Precision.HIGHEST

def matmul(left, right):
    return jnp.dot(left, right, precision=PRECISE, preferred_element_type=left.dtype)

def cholesky_solve(block, right_cols):
    factor = jnp.linalg.cholesky(block)
    partial_value = lax.linalg.triangular_solve(factor, right_cols, left_side=True, lower=True)
    return lax.linalg.triangular_solve(factor, partial_value, left_side=True, lower=True, transpose_a=True)

def couple(lower_gram, upper_gram):
    across_up = upper_gram[:, :RANK]
    across_low = lower_gram[:, :RANK]
    right_up = upper_gram[:, RANK:]
    right_low = lower_gram[:, RANK:]
    schur_block = jnp.eye(RANK, dtype=lower_gram.dtype) - matmul(across_low, across_up)
    target = right_low - matmul(across_low, right_up)
    high_coef = cholesky_solve(matmul(schur_block.T, schur_block), matmul(schur_block.T, target))
    low_coef = right_up - matmul(across_up, high_coef)
    return (low_coef, high_coef)

def leaf_pair(inputs):
    return matmul(inputs[0], inputs[1])

def reference(leaf_inverses, u_bases, v_bases, right_side):
    scales = jnp.asarray(np.repeat(2.0 / (LEAF * 2.0 ** np.arange(LEVELS)), RANK), dtype=u_bases.dtype)
    right_cols = jnp.concatenate([u_bases * scales, right_side], 1).reshape(N_LEAF, LEAF, -1)
    blocks = leaf_inverses.reshape(N_LEAF, LEAF, LEAF)
    carried = lax.map(leaf_pair, (blocks, right_cols))
    v_split = v_bases.reshape(N_LEAF, LEAF, LEVELS * RANK)
    for height in range(1, LEVELS + 1):
        group_size = 2 ** (height - 1)
        columns = carried.shape[2]
        basis_rows = v_split[:, :, (height - 1) * RANK:height * RANK]
        gram_sums = jnp.einsum('plr,plc->prc', basis_rows, carried, precision=PRECISE)
        child_sums = gram_sums.reshape(N_LEAF // group_size, group_size, RANK, columns).sum(1)
        pair_sums = child_sums.reshape(N_LEAF // (2 * group_size), 2, RANK, columns)
        low_coef, high_coef = jax.vmap(couple)(pair_sums[:, 0], pair_sums[:, 1])
        coef_all = jnp.stack([low_coef, high_coef], 1).reshape(N_LEAF // group_size, RANK, columns - RANK)
        coef_leaf = jnp.repeat(coef_all, group_size, axis=0)
        carried = carried[:, :, RANK:] - jnp.einsum('plr,prc->plc', carried[:, :, :RANK], coef_leaf, precision=PRECISE)
    return carried.reshape(N_LEAF * LEAF, RHS)
```

```python
import functools

import jax
import jax.numpy as jnp
from jax import lax
from jax.experimental import pallas as pl
from jax.experimental.pallas import tpu as pltpu
from jax.sharding import PartitionSpec as P

MESH = pl.DeviceIdType.MESH
CHUNKS = 4


def dot(left, right, dims=((1,), (0,))):
    return lax.dot_general(
        left, right, (dims, ((), ())),
        precision=lax.Precision.HIGHEST, preferred_element_type=jnp.float32,
    )


def halves(value):
    high = value.astype(jnp.bfloat16)
    low = (value - high.astype(jnp.float32)).astype(jnp.bfloat16)
    return high, low


def dot3(left, right, dims=((1,), (0,))):
    def one(a, b):
        return lax.dot_general(a, b, (dims, ((), ())), preferred_element_type=jnp.float32)
    return one(left[0], right[1]) + one(left[1], right[0]) + one(left[0], right[0])


def spd_inverse(block, rank):
    rows = lax.broadcasted_iota(jnp.int32, (rank, rank), 0)
    cols = lax.broadcasted_iota(jnp.int32, (rank, rank), 1)
    eye = jnp.where(rows == cols, 1.0, 0.0).astype(jnp.float32)
    wide = jnp.concatenate([block, eye], 1)
    width = 2 * rank
    tiles = tuple(wide[8 * i:8 * i + 8] for i in range(rank // 8))
    sub = lax.broadcasted_iota(jnp.int32, (8, width), 0)

    def eight(_, tiles):
        tiles = list(tiles)
        for k in range(8):
            row = tiles[0][k:k + 1]
            row = row * (1.0 / row[:, k:k + 1])
            new = [t - t[:, k:k + 1] * row for t in tiles]
            new[0] = jnp.where(sub == k, row, new[0])
            tiles = new
        tiles = [pltpu.roll(t, width - 8, 1) for t in tiles]
        return tuple(tiles[1:] + tiles[:1])

    tiles = lax.fori_loop(0, rank // 8, eight, tiles)
    return jnp.concatenate(tiles, 0)[:, :rank]


def kernel(levels, rank, rhs, leaf, dinv_hbm, u_hbm, v_hbm, r_hbm, out_ref, *scratch):
    (dinv, u, v, r, b_hi, b_lo, x, gram, give, coef_ref, load_sem, send_sem, recv_sem) = scratch[:13]
    tp, tw, rest = scratch[13:13 + levels], scratch[13 + levels:13 + 2 * levels], scratch[13 + 2 * levels:]
    me = lax.axis_index("leaf")
    core = lax.rem(me, 2)
    half = rank // 2

    def flipped(bit):
        return me + (1 - 2 * (me // 2 ** bit % 2)) * 2 ** bit

    def flipped_both(bit):
        return flipped(bit) + 1 - 2 * core

    barrier = pltpu.get_barrier_semaphore()
    friends = [flipped(0)]
    for bit in range(1, levels):
        friends += [flipped(bit), flipped_both(bit)]
    for friend in friends:
        pl.semaphore_signal(barrier, inc=1, device_id=(friend,), device_id_type=MESH)

    step = leaf // CHUNKS
    load_u = pltpu.make_async_copy(u_hbm, u, load_sem.at[0])
    load_r = pltpu.make_async_copy(r_hbm, r, load_sem.at[1])
    load_v = pltpu.make_async_copy(v_hbm, v, load_sem.at[2])
    load_d = [
        pltpu.make_async_copy(
            dinv_hbm.at[pl.ds(i * step, step)], dinv.at[pl.ds(i * step, step)], load_sem.at[3 + i]
        )
        for i in range(CHUNKS)
    ]
    load_u.start()
    load_r.start()
    load_d[0].start()
    load_v.start()
    for load in load_d[1:]:
        load.start()

    load_u.wait()
    load_r.wait()
    for i in range(CHUNKS):
        rows = pl.ds(i * step, step)
        parts = [r[rows]]
        for level in range(levels, 0, -1):
            scale = 2.0 / (leaf * 2.0 ** (level - 1))
            parts.append(u[rows, (level - 1) * rank:level * rank] * scale)
        b_hi[rows], b_lo[rows] = halves(jnp.concatenate(parts, 1))

    for i in range(CHUNKS):
        rows = pl.ds(i * step, step)
        load_d[i].wait()
        if i == 0:
            load_v.wait()
        x_part = dot3(halves(dinv[rows]), (b_hi[...], b_lo[...]))
        x[rows] = x_part
        add = dot3(halves(v[rows]), halves(x_part), ((0,), (0,)))
        gram[...] = add if i == 0 else gram[...] + add

    pl.semaphore_wait(barrier, len(friends))

    rows_i = lax.broadcasted_iota(jnp.int32, (rank, rank), 0)
    cols_i = lax.broadcasted_iota(jnp.int32, (rank, rank), 1)
    eye = jnp.where(rows_i == cols_i, 1.0, 0.0).astype(jnp.float32)

    def send(level, slot, src, dst, target):
        copy = pltpu.make_async_remote_copy(
            src_ref=src, dst_ref=dst,
            send_sem=send_sem.at[level - 1, slot], recv_sem=recv_sem.at[level - 1, slot],
            device_id=(target,), device_id_type=MESH,
        )
        copy.start()
        return copy

    def update_rows(cols):
        keep = cols - rank
        coef = halves(coef_ref[:, :keep])
        for i in range(CHUNKS):
            rows = pl.ds(i * step, step)
            taken = halves(x[rows, keep:cols])
            x[rows, :keep] = x[rows, :keep] - dot3(taken, coef)

    copies = []
    state = None
    cols = rhs + levels * rank
    for level in range(1, levels + 1):
        keep = cols - rank
        bit = me // 2 ** (level - 1) % 2
        p_ref, w_ref = tp[level - 1], tw[level - 1]
        far = flipped(level - 1)
        left = levels - level
        rest_copy = None
        if level == 1:
            p_ref[bit] = gram[:rank, keep:]
            w_ref[bit] = gram[:rank, :keep]
            p_copies = [send(1, 0, p_ref.at[bit], p_ref.at[bit], far)]
            w_copies = [send(1, 3, w_ref.at[bit], w_ref.at[bit], far)]
            for which in range(2):
                for m in range(left):
                    give[which, m * half:(m + 1) * half] = gram[pl.ds((m + 1) * rank + which * half, half)]
            rest_copy = send(1, 6, give.at[1 - core], rest[0].at[bit], far)
            rest[0][bit] = give[core]
        else:
            mine = pl.ds(pl.multiple_of(core * half, half), half)
            p_ref[bit, mine] = state[:half, keep:]
            w_ref[bit, mine] = state[:half, :keep]
            p_copies, w_copies = [], []
            targets = [far, flipped_both(level - 1), flipped(0)]
            for slot, target in enumerate(targets):
                p_copies.append(send(level, slot, p_ref.at[bit, mine], p_ref.at[bit, mine], target))
            for slot, target in enumerate(targets):
                w_copies.append(send(level, 3 + slot, w_ref.at[bit, mine], w_ref.at[bit, mine], target))
            if left:
                rest[level - 1][bit] = state[half:]
                rest_copy = send(level, 6, rest[level - 1].at[bit], rest[level - 1].at[bit], far)
            update_rows(cols + rank)
        copies += p_copies + w_copies
        for copy in p_copies:
            copy.wait_recv()
        across_low, across_up = p_ref[0], p_ref[1]
        schur = eye - dot(across_low, across_up)
        inverse = spd_inverse(dot(schur, schur, ((0,), (0,))), rank)
        solver = dot(inverse, schur, ((1,), (1,)))
        for copy in w_copies:
            copy.wait_recv()
        right_up = w_ref[1]
        high_coef = dot(solver, w_ref[0] - dot(across_low, right_up))
        low_coef = right_up - dot(across_up, high_coef)
        if left:
            copies.append(rest_copy)
            rest_copy.wait_recv()
            rest_ref = rest[level - 1]
            state = (
                (rest_ref[0, :, :keep] - dot(rest_ref[0, :, keep:], low_coef))
                + (rest_ref[1, :, :keep] - dot(rest_ref[1, :, keep:], high_coef))
            )
        coef_ref[:, :keep] = jnp.where(bit == 1, high_coef, low_coef)
        cols = keep

    coef = halves(coef_ref[:, :rhs])
    for i in range(CHUNKS):
        rows = pl.ds(i * step, step)
        out_ref[rows] = x[rows, :rhs] - dot3(halves(x[rows, rhs:rhs + rank]), coef)
    for copy in copies:
        copy.wait_send()


def body(leaf_inverses, u_bases, v_bases, right_side):
    leaf = leaf_inverses.shape[0]
    levels = lax.axis_size("leaf").bit_length() - 1
    rank = u_bases.shape[1] // levels
    rhs = right_side.shape[1]
    cols = rhs + levels * rank
    half = rank // 2
    f32 = jnp.float32
    scratch = [
        pltpu.VMEM(leaf_inverses.shape, f32),
        pltpu.VMEM(u_bases.shape, f32),
        pltpu.VMEM(v_bases.shape, f32),
        pltpu.VMEM(right_side.shape, f32),
        pltpu.VMEM((leaf, cols), jnp.bfloat16),
        pltpu.VMEM((leaf, cols), jnp.bfloat16),
        pltpu.VMEM((leaf, cols), f32),
        pltpu.VMEM((levels * rank, cols), f32),
        pltpu.VMEM((2, (levels - 1) * half, cols), f32),
        pltpu.VMEM((rank, cols - rank), f32),
        pltpu.SemaphoreType.DMA((3 + CHUNKS,)),
        pltpu.SemaphoreType.DMA((levels, 7)),
        pltpu.SemaphoreType.DMA((levels, 7)),
    ]
    widths = [cols - i * rank for i in range(levels)]
    scratch += [pltpu.VMEM((2, rank, rank), f32) for _ in widths]
    scratch += [pltpu.VMEM((2, rank, w - rank), f32) for w in widths]
    scratch += [
        pltpu.VMEM((2, (levels - 1 - i) * half, w), f32) for i, w in enumerate(widths[:-1])
    ]
    return pl.pallas_call(
        functools.partial(kernel, levels, rank, rhs, leaf),
        out_shape=jax.ShapeDtypeStruct(right_side.shape, f32),
        in_specs=[pl.BlockSpec(memory_space=pl.ANY)] * 4,
        out_specs=pl.BlockSpec(memory_space=pltpu.VMEM),
        scratch_shapes=scratch,
        compiler_params=pltpu.CompilerParams(
            collective_id=0, has_side_effects=True, vmem_limit_bytes=48 * 2**20
        ),
        name="tree_solve",
    )(leaf_inverses, u_bases, v_bases, right_side)


def solution(mesh):
    in_specs = (P("leaf", None), P("leaf", None), P("leaf", None), P("leaf", None))
    out_specs = P("leaf", None)
    return jax.shard_map(body, mesh=mesh, in_specs=in_specs, out_specs=out_specs, check_vma=False)
```

```python
import functools

import jax
import jax.numpy as jnp
from jax import lax
from jax.experimental import pallas as pl
from jax.experimental.pallas import tpu as pltpu
from jax.sharding import PartitionSpec as P

MESH = pl.DeviceIdType.MESH
CHUNKS = 4


def dot(left, right, dims=((1,), (0,))):
    return lax.dot_general(
        left, right, (dims, ((), ())),
        precision=lax.Precision.HIGHEST, preferred_element_type=jnp.float32,
    )


def halves(value):
    high = value.astype(jnp.bfloat16)
    low = (value - high.astype(jnp.float32)).astype(jnp.bfloat16)
    return high, low


def dot3(left, right, dims=((1,), (0,))):
    def one(a, b):
        return lax.dot_general(a, b, (dims, ((), ())), preferred_element_type=jnp.float32)
    return one(left[0], right[1]) + one(left[1], right[0]) + one(left[0], right[0])


def spd_inverse(block, rank):
    rows = lax.broadcasted_iota(jnp.int32, (rank, rank), 0)
    cols = lax.broadcasted_iota(jnp.int32, (rank, rank), 1)
    eye = jnp.where(rows == cols, 1.0, 0.0).astype(jnp.float32)
    wide = jnp.concatenate([block, eye], 1)
    width = 2 * rank
    tiles = tuple(wide[8 * i:8 * i + 8] for i in range(rank // 8))
    sub = lax.broadcasted_iota(jnp.int32, (8, width), 0)

    def eight(_, tiles):
        tiles = list(tiles)
        for k in range(8):
            row = tiles[0][k:k + 1]
            row = row * (1.0 / row[:, k:k + 1])
            new = [t - t[:, k:k + 1] * row for t in tiles]
            new[0] = jnp.where(sub == k, row, new[0])
            tiles = new
        tiles = [pltpu.roll(t, width - 8, 1) for t in tiles]
        return tuple(tiles[1:] + tiles[:1])

    tiles = lax.fori_loop(0, rank // 8, eight, tiles)
    return jnp.concatenate(tiles, 0)[:, :rank]


def leaf_kernel(levels, rank, rhs, leaf, dinv, u_t, v_t, r, x, gram, b_hi, b_lo):
    index = pl.program_id(0)
    keep = levels * rank

    @pl.when(index == 0)
    def _():
        b_hi[:, :rhs], b_lo[:, :rhs] = halves(r[...])
        parts = []
        for level in range(levels, 0, -1):
            scale = 2.0 / (leaf * 2.0 ** (level - 1))
            parts.append(u_t[(level - 1) * rank:level * rank] * scale)
        b_hi[:, rhs:], b_lo[:, rhs:] = halves(jnp.concatenate(parts, 0).T)
        gram[...] = jnp.zeros_like(gram)

    part = dot3(halves(dinv[...]), (b_hi[...], b_lo[...]))
    x[...] = part
    gram[...] += dot3(halves(v_t[...]), halves(part))


def final_kernel(rhs, x, comp, out):
    out[...] = x[:, :rhs] + dot3(halves(x[:, rhs:]), halves(comp[...]))


def kernel(levels, rank, rhs, gram, comp, *scratch):
    give, send_sem, recv_sem = scratch[:3]
    groups = [scratch[3 + i * levels:3 + (i + 1) * levels] for i in range(4)]
    tp, tw, low_refs, high_refs = groups
    near_refs = scratch[3 + 4 * levels:3 + 4 * levels + levels - 1]
    far_refs = scratch[3 + 4 * levels + levels - 1:]
    me = lax.axis_index("leaf")
    core = lax.rem(me, 2)
    half = rank // 2

    def flipped(bit):
        return me + (1 - 2 * (me // 2 ** bit % 2)) * 2 ** bit

    def flipped_both(bit):
        return flipped(bit) + 1 - 2 * core

    barrier = pltpu.get_barrier_semaphore()
    friends = [flipped(0)]
    for bit in range(1, levels):
        friends += [flipped(bit), flipped_both(bit)]
    for friend in friends:
        pl.semaphore_signal(barrier, inc=1, device_id=(friend,), device_id_type=MESH)
    pl.semaphore_wait(barrier, len(friends))

    rows_i = lax.broadcasted_iota(jnp.int32, (rank, rank), 0)
    cols_i = lax.broadcasted_iota(jnp.int32, (rank, rank), 1)
    eye = jnp.where(rows_i == cols_i, 1.0, 0.0).astype(jnp.float32)

    def send(level, slot, src, dst, target):
        copy = pltpu.make_async_remote_copy(
            src_ref=src, dst_ref=dst,
            send_sem=send_sem.at[level - 1, slot], recv_sem=recv_sem.at[level - 1, slot],
            device_id=(target,), device_id_type=MESH,
        )
        copy.start()
        return copy

    def merged(ref, level, keep):
        return (
            (ref[0, :, :keep] - dot(ref[0, :, keep:], low_refs[level - 1][...]))
            + (ref[1, :, :keep] - dot(ref[1, :, keep:], high_refs[level - 1][...]))
        )

    copies = []
    far_copy = None
    top = None
    cols = rhs + levels * rank
    for level in range(1, levels + 1):
        keep = cols - rank
        bit = me // 2 ** (level - 1) % 2
        p_ref, w_ref = tp[level - 1], tw[level - 1]
        other = flipped(level - 1)
        left = levels - level
        near_copy = None
        next_far = None
        if level == 1:
            p_ref[bit] = gram[:rank, keep:]
            w_ref[bit] = gram[:rank, :keep]
            p_copies = [send(1, 0, p_ref.at[bit], p_ref.at[bit], other)]
            w_copies = [send(1, 3, w_ref.at[bit], w_ref.at[bit], other)]
            for which in range(2):
                for m in range(left):
                    give[which, m * half:(m + 1) * half] = gram[pl.ds((m + 1) * rank + which * half, half)]
            near_copy = send(1, 6, give.at[1 - core, pl.ds(0, half)], near_refs[0].at[bit], other)
            near_refs[0][bit] = give[core, :half]
            if left > 1:
                rows = pl.ds(half, (left - 1) * half)
                next_far = send(1, 7, give.at[1 - core, rows], far_refs[0].at[bit], other)
                far_refs[0][bit] = give[core, half:]
        else:
            mine = pl.ds(pl.multiple_of(core * half, half), half)
            p_ref[bit, mine] = top[:, keep:]
            w_ref[bit, mine] = top[:, :keep]
            p_copies, w_copies = [], []
            targets = [other, flipped_both(level - 1), flipped(0)]
            for slot, target in enumerate(targets):
                p_copies.append(send(level, slot, p_ref.at[bit, mine], p_ref.at[bit, mine], target))
            for slot, target in enumerate(targets):
                w_copies.append(send(level, 3 + slot, w_ref.at[bit, mine], w_ref.at[bit, mine], target))
            if left:
                far_copy.wait_recv()
                state = merged(far_refs[level - 2], level - 1, cols)
                near_ref = near_refs[level - 1]
                near_ref[bit] = state[:half]
                near_copy = send(level, 6, near_ref.at[bit], near_ref.at[bit], other)
                if left > 1:
                    far_ref = far_refs[level - 1]
                    far_ref[bit] = state[half:]
                    next_far = send(level, 7, far_ref.at[bit], far_ref.at[bit], other)
        far_copy = next_far
        copies += p_copies + w_copies + [c for c in (near_copy, next_far) if c is not None]
        for copy in p_copies:
            copy.wait_recv()
        across_low, across_up = p_ref[0], p_ref[1]
        schur = eye - dot(across_low, across_up)
        inverse = spd_inverse(dot(schur, schur, ((0,), (0,))), rank)
        solver = dot(inverse, schur, ((1,), (1,)))
        for copy in w_copies:
            copy.wait_recv()
        right_up = w_ref[1]
        high_coef = dot(solver, w_ref[0] - dot(across_low, right_up))
        low_refs[level - 1][...] = right_up - dot(across_up, high_coef)
        high_refs[level - 1][...] = high_coef
        if left:
            near_copy.wait_recv()
            top = merged(near_refs[level - 1], level, keep)
        cols = keep

    for level in range(levels, 0, -1):
        bit = me // 2 ** (level - 1) % 2
        coef = jnp.where(bit == 1, high_refs[level - 1][...], low_refs[level - 1][...])
        done = (levels - level) * rank
        value = coef[:, :rhs]
        if done:
            value = value + dot(coef[:, rhs:], comp[:done])
        comp[done:done + rank] = -value
    for copy in copies:
        copy.wait_send()


def body(leaf_inverses, u_bases, v_bases, right_side):
    leaf = leaf_inverses.shape[0]
    levels = lax.axis_size("leaf").bit_length() - 1
    rank = u_bases.shape[1] // levels
    rhs = right_side.shape[1]
    inner = levels * rank
    cols = rhs + inner
    half = rank // 2
    step = leaf // CHUNKS
    f32 = jnp.float32
    x, gram = pl.pallas_call(
        functools.partial(leaf_kernel, levels, rank, rhs, leaf),
        grid=(CHUNKS,),
        out_shape=[jax.ShapeDtypeStruct((leaf, cols), f32), jax.ShapeDtypeStruct((inner, cols), f32)],
        in_specs=[
            pl.BlockSpec((step, leaf), lambda i: (i, 0)),
            pl.BlockSpec((inner, leaf), lambda i: (0, 0)),
            pl.BlockSpec((inner, step), lambda i: (0, i)),
            pl.BlockSpec((leaf, rhs), lambda i: (0, 0)),
        ],
        out_specs=[
            pl.BlockSpec((step, cols), lambda i: (i, 0)),
            pl.BlockSpec((inner, cols), lambda i: (0, 0)),
        ],
        scratch_shapes=[pltpu.VMEM((leaf, cols), jnp.bfloat16)] * 2,
        compiler_params=pltpu.CompilerParams(vmem_limit_bytes=40 * 2**20),
        name="leaf_products",
    )(leaf_inverses, u_bases.T, v_bases.T, right_side)

    widths = [cols - i * rank for i in range(levels)]
    scratch = [
        pltpu.VMEM((2, (levels - 1) * half, cols), f32),
        pltpu.SemaphoreType.DMA((levels, 8)),
        pltpu.SemaphoreType.DMA((levels, 8)),
    ]
    scratch += [pltpu.VMEM((2, rank, rank), f32) for _ in widths]
    scratch += [pltpu.VMEM((2, rank, w - rank), f32) for w in widths]
    scratch += [pltpu.VMEM((rank, w - rank), f32) for w in widths] * 2
    scratch += [pltpu.VMEM((2, half, w), f32) for w in widths[:-1]]
    scratch += [
        pltpu.VMEM((2, (levels - 2 - i) * half, w), f32) for i, w in enumerate(widths[:-2])
    ]
    comp = pl.pallas_call(
        functools.partial(kernel, levels, rank, rhs),
        out_shape=jax.ShapeDtypeStruct((inner, rhs), f32),
        in_specs=[pl.BlockSpec(memory_space=pltpu.VMEM)],
        out_specs=pl.BlockSpec(memory_space=pltpu.VMEM),
        scratch_shapes=scratch,
        compiler_params=pltpu.CompilerParams(
            collective_id=0, has_side_effects=True, vmem_limit_bytes=32 * 2**20
        ),
        name="tree_solve",
    )(gram)

    return pl.pallas_call(
        functools.partial(final_kernel, rhs),
        grid=(CHUNKS,),
        out_shape=jax.ShapeDtypeStruct((leaf, rhs), f32),
        in_specs=[
            pl.BlockSpec((step, cols), lambda i: (i, 0)),
            pl.BlockSpec((inner, rhs), lambda i: (0, 0)),
        ],
        out_specs=pl.BlockSpec((step, rhs), lambda i: (i, 0)),
        name="leaf_solution",
    )(x, comp)


def solution(mesh):
    in_specs = (P("leaf", None), P("leaf", None), P("leaf", None), P("leaf", None))
    out_specs = P("leaf", None)
    return jax.shard_map(body, mesh=mesh, in_specs=in_specs, out_specs=out_specs, check_vma=False)
```
